32 devices in a mesh: ops: 8 (over z, core), blk: 4 (over y, x).
Axes of the slice: x: 2, y: 2, z: 4, core: 2. Of those that a mesh axis runs over, the one named last changes fastest.
Arguments:
- psi: bfloat16 [2048, 1024], P('blk'), may hold values from -6 to 6
- left_blocks: bfloat16 [64, 16, 128, 128], P('ops', 'blk'), may hold values from -0.5 to 0.5
- right_ops: bfloat16 [64, 1024, 1024], P(('ops', 'blk')), may hold values from -0.046875 to 0.046875
- block_target: int32 [64, 16], P('ops'), may hold values from 0 to 15
- left_partner: int32 [64], P('ops'), may hold values from 0 to 63, as said below
- block_len: int32 [16], replicated, may hold values from 1 to 128, 1536 in all
Outputs:
- sigma: bfloat16 [2048, 1024], P('blk', 'ops')
The draws below stay inside these ranges and needn't reach their ends.
Inputs may be any that keep to these rules, and one draw needn't show every extreme that they name: left_partner is a permutation of 0 to 63 that maps each aligned group of 8 operators onto itself.
All inputs are finite; a program needn't handle non-finite values.
Results may differ from the reference program's by a relative error of at most 0.018.
Values may be sent and summed in bfloat16 or wider, within the bound.
No kernel may reach another device: no remote copies, remote signals or barrier semaphores. Data moves between devices by JAX's collectives and lax.ppermute only.
A program may use at most 128 MiB of HBM per device.

```python
import math
import jax
import jax.numpy as jnp
import numpy as np
from jax import lax

BOND = 2048
BS = 128
RW = 1024
NB = 16
K = 64
OPS_GROUP = 8


def draw_left_partner(key, part):
    scores = jax.random.randint(key, (K,), 0, 65536, dtype=jnp.int32) * K + jnp.arange(K, dtype=jnp.int32)
    groups = K // OPS_GROUP
    order = jnp.argsort(scores.reshape(groups, OPS_GROUP), axis=1, stable=True).astype(jnp.int32)
    shifted = order + jnp.arange(groups, dtype=jnp.int32)[:, None] * OPS_GROUP
    return shifted.reshape(K).astype(jnp.int32)


def with_ends(values, stream_key, low, top_value):
    extent = values.shape
    place = [jax.random.randint(jax.random.fold_in(stream_key, axis), (), 0, extent[axis]) for axis in range(len(extent))]
    values = values.at[tuple(place)].set(low)
    longest = extent.index(max(extent))
    place[longest] = (place[longest] + 1) % extent[longest]
    return values.at[tuple(place)].set(top_value)


def with_spikes(array, rng, source, target, parts, factor):
    owner, partner = [(jnp.arange(array.shape[axis_at]) // (array.shape[axis_at] // parts)).reshape([-1 if axis == axis_at else 1 for axis in range(array.ndim)]) for axis_at in (source, target)]
    chosen = jax.random.permutation(rng, parts)[partner]
    strong = (owner == chosen) | (owner == (partner + parts // 2) % parts)
    return jnp.where(strong, factor * array, array)


def level_of(key, extent, split, smallest, top_value):
    factor_of = 1.0
    for position, parts in split:
        draws = jax.random.uniform(jax.random.fold_in(jax.random.fold_in(key, 6), position), (parts,), jnp.float32, smallest / len(split), top_value / len(split))
        factor_of = factor_of * jnp.repeat(jnp.exp(draws), extent[position] // parts).reshape((-1,) + (1,) * (len(extent) - 1 - position))
    return factor_of


def profile(count, total, reach, skew):
    weights = [(1 << 20) // math.isqrt(rank ** skew) + 1 for rank in range(2, count + 1)]
    surplus, holding = total - reach - (count - 1), [1] * (count - 1)
    while surplus > 0:
        candidates = [i for i in range(count - 1) if holding[i] < reach]
        mass, remaining = sum([weights[i] for i in candidates]), surplus
        for i in candidates:
            more = min(reach - holding[i], max(1, remaining * weights[i] // mass), surplus)
            holding[i] = holding[i] + more
            surplus = surplus - more
    return np.array([reach] + holding)


def uneven_parts(stream_key, amount, total, bound, skew):
    if amount == 2:
        one = jax.random.randint(stream_key, (), max(1, total - bound), min(bound, total - 1) + 1)
        return jnp.stack([one, total - one])
    lengths = jnp.asarray(profile(amount, total, bound, skew), jnp.int32)
    couples = (amount - 1) // 2
    source_of, taker = lengths[1:1 + 2 * couples:2], lengths[2:2 + 2 * couples:2]
    room = jnp.minimum(source_of - 1, bound - taker)
    moved = jax.random.randint(jax.random.fold_in(stream_key, 1), (couples,), 0, 1 << 20) % (room + 1)
    lengths = lengths.at[1:1 + 2 * couples:2].set(source_of - moved).at[2:2 + 2 * couples:2].set(taker + moved)
    return lengths[jax.random.permutation(jax.random.fold_in(stream_key, 2), amount)]


def noise(own_key, extent, scale, reach, shards=(), held_as=jnp.bfloat16):
    gain = level_of(own_key, extent, shards, -0.22, 0.18) if shards else 1.0
    values = jax.random.normal(own_key, extent, jnp.float32) * scale * gain
    return jnp.minimum(jnp.maximum(values, -reach), reach).astype(held_as)


def gaussian_with(own_key, shape, spread, limit, shards, heavy, kind=jnp.bfloat16):
    drawn = spread * jax.random.normal(own_key, shape, jnp.float32)
    if shards:
        drawn = drawn * level_of(own_key, shape, shards, -0.22, 0.18)
    return jnp.clip(with_spikes(drawn, jax.random.fold_in(own_key, 3), *heavy), -limit, limit).astype(kind)


def setup_inputs(seed: int = 0) -> dict:
    streams_of = jax.random.split(jax.random.key(seed), 7)
    psi = noise(streams_of[0], (BOND, RW), 1.0, 6.0, ((0, 4),))
    left_blocks = noise(streams_of[1], (K, NB, BS, BS), BS ** -0.5, 0.5, ((0, 8), (1, 4)))
    right_ops = gaussian_with(streams_of[2], (K, RW, RW), (RW * K) ** -0.5, 0.046875, ((0, 32),), (0, 2, 32, 2.75))
    block_target = with_ends(jax.random.randint(streams_of[3], (K, NB), 0, NB), jax.random.fold_in(streams_of[3], 1), 0, NB - 1).astype(jnp.int32)
    left_partner = draw_left_partner(jax.random.fold_in(streams_of[6], 71), 0)
    block_len = uneven_parts(streams_of[5], NB, 3 * BOND // 4, BS, 2).astype(jnp.int32)
    return dict(psi=psi, left_blocks=left_blocks, right_ops=right_ops, block_target=block_target, left_partner=left_partner, block_len=block_len)


def reference(psi, left_blocks, right_ops, block_target, left_partner, block_len):
    nblocks = BOND // BS
    row_index = jnp.arange(BS, dtype=jnp.int32)
    live_rows = row_index[None, :] < block_len[:, None]
    masked = psi.reshape(nblocks, BS, RW) * live_rows[:, :, None].astype(jnp.bfloat16)
    states = masked.reshape(BOND, RW).astype(jnp.float32)

    def absorb(totals, index):
        image = jnp.dot(states, right_ops[index].astype(jnp.float32), precision=lax.Precision.HIGHEST)
        image = lax.optimization_barrier(image.astype(jnp.bfloat16)).astype(jnp.float32)
        image = image.reshape(nblocks, BS, RW)
        owner = left_partner[index]
        mixed = jnp.einsum("qab,qbr->qar", left_blocks[owner].astype(jnp.float32), image, precision=lax.Precision.HIGHEST)
        totals = totals + jax.ops.segment_sum(mixed, block_target[owner], num_segments=nblocks)
        return totals, None

    start = jnp.zeros((nblocks, BS, RW), jnp.float32)
    totals = lax.scan(absorb, start, jnp.arange(K, dtype=jnp.int32))[0]
    result = totals * live_rows[:, :, None].astype(jnp.float32)
    return result.reshape(BOND, RW).astype(jnp.bfloat16)
```

```python
import functools

import jax
import jax.numpy as jnp
from jax import lax
from jax.experimental import pallas as pl
from jax.experimental.pallas import tpu as pltpu
from jax.sharding import PartitionSpec as P

BF16, F32 = jnp.bfloat16, jnp.float32


def rev(mask, bits):
    out = 0
    for k in range(bits):
        out = out | (((mask >> k) & 1) << (bits - 1 - k))
    return out


def turn(core, mask, bits):
    return jnp.where(core == 0, mask, rev(mask, bits))


def pick_kernel(bits, local_ops, group_size, partner, lens, left, *outs):
    me, ops = lax.axis_index("blk"), lax.axis_index("ops")
    core = lax.rem(ops, 2)
    blocks, rows = left.shape[1], left.shape[2]
    lane = lax.broadcasted_iota(jnp.int32, (rows, rows), 1)
    for m, out in enumerate(outs):
        dest = me ^ turn(core, m, bits)
        for s in range(local_ops):
            own = partner[dest * local_ops + s] - ops * group_size
            for i in range(blocks):
                value = left[own, i].astype(F32)
                out[s, i] = jnp.where(lane < lens[me * blocks + i], value, 0.0).astype(BF16)


def mix_kernel(bits, local_ops, group_size, target, partner, *refs):
    n = 1 << bits
    lefts, refs = refs[:n], refs[n:]
    images, (keep, send, acc) = refs[:-3], refs[-3:]
    me, ops = lax.axis_index("blk"), lax.axis_index("ops")
    core = lax.rem(ops, 2)
    blocks, rows = lefts[0].shape[1], lefts[0].shape[2]
    half = blocks // 2
    acc[...] = jnp.zeros_like(acc)
    for s in range(local_ops):
        own = partner[me * local_ops + s] - ops * group_size
        own_images = images[s * (2 * n - 1):(s + 1) * (2 * n - 1)]
        work = [(0, i, own_images[0], i) for i in range(blocks)]
        for m in range(1, n):
            work += [(m, core * half + i, own_images[m], i) for i in range(half)]
            work += [(rev(m, bits), (1 - core) * half + i, own_images[n - 1 + m], i) for i in range(half)]
        for m, i, image, j in work:
            source = (me ^ turn(core, m, bits)) * blocks + i
            t = target[own, source]
            hop = (t // blocks) ^ me
            slot = hop * blocks + lax.rem(t, blocks)
            mixed = jnp.dot(
                lefts[m][s, i], image[j * rows:(j + 1) * rows, :], preferred_element_type=F32
            )
            acc[slot] += mixed
    width = acc.shape[-1] // 2
    for j in range(n):
        for i in range(blocks):
            at = pl.ds(i * rows, rows)
            mine = acc[jnp.where(core == 0, rev(j, bits), j) * blocks + i]
            theirs = acc[jnp.where(core == 0, j, rev(j, bits)) * blocks + i]
            keep[0, j, at, :] = jnp.where(core == 0, mine[:, :width], mine[:, width:])
            send[0, j, at, :] = jnp.where(core == 0, theirs[:, width:], theirs[:, :width]).astype(BF16)


def local(nops, nblk, psi, left_blocks, right_ops, block_target, left_partner, block_len):
    bits = nblk.bit_length() - 1
    nz = nops // 2
    group_size, blocks, rows = left_blocks.shape[:3]
    local_ops = right_ops.shape[0]
    height, columns = psi.shape
    half = height // 2
    width = columns // nops
    me, ops = lax.axis_index("blk"), lax.axis_index("ops")
    core = lax.rem(ops, 2)
    smem = pl.BlockSpec(memory_space=pltpu.SMEM)
    vmem = pl.BlockSpec(memory_space=pltpu.VMEM)

    def across(x, k):
        pairs = [
            (o * nblk + b, o * nblk + (b ^ ((1 << k) if o % 2 == 0 else rev(1 << k, bits))))
            for o in range(nops) for b in range(nblk)
        ]
        return lax.ppermute(x, ("ops", "blk"), pairs)

    def direct(x, m):
        pairs = [
            (o * nblk + b, o * nblk + (b ^ (m if o % 2 == 0 else rev(m, bits))))
            for o in range(nops) for b in range(nblk)
        ]
        return lax.ppermute(x, ("ops", "blk"), pairs)

    def partner_core(x):
        return lax.ppermute(x, "ops", [(o, o ^ 1) for o in range(nops)])

    def along_z(x, m):
        return lax.ppermute(x, "ops", [(o, o ^ (2 * m)) for o in range(nops)])

    chunks = [lax.dynamic_slice_in_dim(psi, core * half, half, 0)]
    for m in range(1, nblk):
        k = m.bit_length() - 1
        chunks.append(across(chunks[m ^ (1 << k)], k))
    others = [partner_core(c) for c in chunks[1:]]

    picked = pl.pallas_call(
        functools.partial(pick_kernel, bits, local_ops, group_size),
        out_shape=[jax.ShapeDtypeStruct((local_ops, blocks, rows, rows), BF16)] * nblk,
        in_specs=[smem, smem, vmem],
        out_specs=[vmem] * nblk,
        name="pick",
    )(left_partner, block_len, left_blocks)
    lefts = [picked[0]] + [direct(picked[m], m) for m in range(1, nblk)]

    sources = [psi] + chunks[1:] + others
    images = [
        [jnp.dot(c, right_ops[s], preferred_element_type=F32).astype(BF16) for c in sources]
        for s in range(local_ops)
    ]

    def mix(zs):
        def column(i):
            z = lax.axis_index("ops") // 2
            return z ^ (i + zs[0])

        in_specs = [smem, smem] + [vmem] * nblk
        operands = [block_target, left_partner] + lefts
        for s in range(local_ops):
            for image in images[s]:
                in_specs.append(pl.BlockSpec((image.shape[0], 2 * width), lambda i: (0, column(i))))
                operands.append(image)
        out = (len(zs), nblk, blocks * rows, width)
        spec = pl.BlockSpec((1,) + out[1:], lambda i: (i, 0, 0, 0))
        return pl.pallas_call(
            functools.partial(mix_kernel, bits, local_ops, group_size),
            grid=(len(zs),),
            out_shape=[jax.ShapeDtypeStruct(out, F32), jax.ShapeDtypeStruct(out, BF16)],
            in_specs=in_specs,
            out_specs=[spec, spec],
            scratch_shapes=[pltpu.VMEM((nblk * blocks, rows, 2 * width), F32)],
            name=f"mix{zs[0]}",
        )(*operands)

    result = None
    groups = [list(range(nz // 2, nz)), list(range(nz // 2))]
    parts = []
    for zs in groups:
        keep, send = mix(zs)
        current = keep + partner_core(send).astype(F32)
        for k in range(bits):
            size = current.shape[1] // 2
            current = current[:, :size] + across(current[:, size:].astype(BF16), k).astype(F32)
        for i, m in enumerate(zs):
            part = current[i, 0]
            parts.append(along_z(part.astype(BF16), m).astype(F32) if m else part)
    result = functools.reduce(jnp.add, parts)
    row_index = jnp.arange(rows, dtype=jnp.int32)
    own_len = lax.dynamic_slice_in_dim(block_len, me * blocks, blocks, 0)
    live = (row_index[None, :] < own_len[:, None]).astype(F32)
    result = result.reshape(blocks, rows, width) * live[:, :, None]
    return result.reshape(height, width).astype(BF16)


def solution(mesh):
    nops, nblk = mesh.shape["ops"], mesh.shape["blk"]
    return jax.shard_map(
        functools.partial(local, nops, nblk),
        mesh=mesh,
        in_specs=(
            P("blk", None),
            P("ops", "blk", None, None),
            P(("ops", "blk"), None, None),
            P("ops", None),
            P("ops"),
            P(),
        ),
        out_specs=P("blk", "ops"),
        check_vma=False,
    )
```
